32 devices in a mesh: aux: 8 (over z, x), lmo: 4 (over y, core).
Axes of the slice: x: 2, y: 2, z: 4, core: 2. Of those that a mesh axis runs over, the one named last changes fastest.
Arguments:
- aux_ints: bfloat16 [256, 768, 768], P(('aux', 'lmo')), may hold values from -6 to 6
- lmo_coef: bfloat16 [128, 384], P(('aux', 'lmo')), may hold values from -0.3125 to 0.3125
- ao_domain: int32 [128, 3], replicated, may hold values from 0 to 5, as said below
- ao_count: int32 [128], replicated, may hold values from 1 to 3
- pao_domain: int32 [128, 3], replicated, may hold values from 0 to 5, as said below
- pao_count: int32 [128], replicated, may hold values from 1 to 3, as said below
- owner_order: int32 [128], replicated, may hold values from 0 to 127, as said below
- pao_coef: bfloat16 [128, 384, 256], P(('aux', 'lmo')), may hold values from -0.3125 to 0.3125
Outputs:
- pair_ints: bfloat16 [128, 256, 256], P(('aux', 'lmo'))
- pair_metric: float32 [128, 256, 256], P(('aux', 'lmo'))
The draws below stay inside these ranges and needn't reach their ends.
Inputs may be any that keep to these rules, and one draw needn't show every extreme that they name: `ao_domain`: each row holds 3 different block numbers; slots from ao_count on are unused. `pao_domain`: each row holds 3 different block numbers; slots from pao_count on are unused. `pao_count`: the LMOs of the 4 owner slots of one device use together at most 8 PAO block slots, and those of some device use exactly 8. `owner_order`: every LMO stands in exactly one slot.
All inputs are finite; a program needn't handle non-finite values.
Results may differ from the reference program's by a relative error of at most 0.0049.
Values may be sent and summed in bfloat16 or wider, within the bound.
No kernel may reach another device: no remote copies, remote signals or barrier semaphores. Data moves between devices by JAX's collectives and lax.ppermute only.
A program may use at most 128 MiB of HBM per device.

```python
import jax
import jax.numpy as jnp
from jax import lax

BLK = 128
NBA = 6
DB = 3
PB = 3
NPAO = 256
P_D = 8
LMO_DEV = 4
AO = 768
NAUX = 256
NLMO = 128
USED = 8


def draw_rows(key, row_depth):
    subkeys = jax.random.split(key, NLMO)

    def one_row(subkey):
        return jax.random.permutation(subkey, NBA)[:row_depth]
    return jax.vmap(one_row)(subkeys).astype(jnp.int32)


def draw_ao_domain(key, part):
    return draw_rows(jax.random.fold_in(key, 11), DB)


def draw_pao_domain(key, part):
    return draw_rows(jax.random.fold_in(key, 23), PB)


def owner_tables(key):
    base = jax.random.fold_in(key, 31)
    order_key, target_key, full_key, unit_key = jax.random.split(base, 4)
    order = jax.random.permutation(order_key, NLMO).astype(jnp.int32)
    groups = NLMO // LMO_DEV
    target = jax.random.randint(target_key, (groups,), LMO_DEV, USED + 1).astype(jnp.int32)
    full_group = jax.random.randint(full_key, (), 0, groups).astype(jnp.int32)
    target = jnp.where(jnp.arange(groups, dtype=jnp.int32) == full_group, USED, target)
    counts = jnp.ones((groups, LMO_DEV), jnp.int32)
    members = jnp.arange(LMO_DEV, dtype=jnp.int32)
    for unit in range(USED - LMO_DEV):
        scores = jax.random.randint(jax.random.fold_in(unit_key, unit), (groups, LMO_DEV), 0, 1 << 20).astype(jnp.int32)
        scores = scores * LMO_DEV + members[None, :]
        scores = jnp.where(counts < PB, scores, -1)
        picked = jnp.argmax(scores, axis=1).astype(jnp.int32)
        adding = (members[None, :] == picked[:, None]) & (unit < target - LMO_DEV)[:, None]
        counts = counts + adding.astype(jnp.int32)
    by_slot = counts.reshape(NLMO)
    pao_count = jnp.zeros((NLMO,), jnp.int32).at[order].set(by_slot)
    return (order, pao_count)


def draw_owner_order(key, part):
    return owner_tables(key)[0]


def draw_pao_count(key, part):
    return owner_tables(key)[1]


def set_ends(entries, stream_key, low, high):
    longest = entries.shape.index(max(entries.shape))
    spots = []
    for shift in (0, 1):
        where = [jax.random.randint(jax.random.fold_in(stream_key, axis), (), 0, length) for axis, length in enumerate(entries.shape)]
        where[longest] = (where[longest] + shift) % entries.shape[longest]
        spots.append(tuple(where))
    return entries.at[spots[0]].set(low).at[spots[1]].set(high)


def shard_levels(stream_key, shape, shards, least, high):
    factor_of, own = 1.0, jax.random.fold_in(stream_key, 6)
    for position, shards_of in shards:
        steps = jnp.exp(jax.random.uniform(jax.random.fold_in(own, position), (shards_of,), jnp.float32, least / len(shards), high / len(shards)))
        factor_of = factor_of * jnp.repeat(steps, shape[position] // shards_of).reshape([-1 if axis == position else 1 for axis in range(len(shape))])
    return factor_of


def gaussian(stream_key, dims, spread, reach, cuts=(), kind=jnp.bfloat16):
    values = jax.random.normal(stream_key, dims, jnp.float32) * spread
    if len(cuts) > 0:
        values = shard_levels(stream_key, dims, cuts, -0.22, 0.18) * values
    return jnp.clip(values, min=-reach, max=reach).astype(kind)


def setup_inputs(seed: int = 0) -> dict:
    streams_of = jax.random.split(jax.random.key(seed), 9)
    aux_ints = gaussian(streams_of[0], (NAUX, AO, AO), 1.0, 6.0, ((0, 32),))
    lmo_coef = gaussian(streams_of[1], (NLMO, DB * BLK), (DB * BLK) ** -0.5, 0.3125, ((0, 32),))
    ao_domain = draw_ao_domain(jax.random.fold_in(streams_of[8], 71), 0)
    ao_count = set_ends(jax.random.randint(streams_of[3], (NLMO,), 1, DB + 1), jax.random.fold_in(streams_of[3], 1), 1, DB).astype(jnp.int32)
    pao_domain = draw_pao_domain(jax.random.fold_in(streams_of[8], 71), 0)
    pao_count = draw_pao_count(jax.random.fold_in(streams_of[8], 71), 0)
    owner_order = draw_owner_order(jax.random.fold_in(streams_of[8], 71), 0)
    pao_coef = gaussian(streams_of[7], (NLMO, PB * BLK, NPAO), (PB * BLK) ** -0.5, 0.3125, ((0, 32),))
    return dict(aux_ints=aux_ints, lmo_coef=lmo_coef, ao_domain=ao_domain, ao_count=ao_count, pao_domain=pao_domain, pao_count=pao_count, owner_order=owner_order, pao_coef=pao_coef)


def place(lmo_coef, domain, block_count, blocks):
    lmo_total = lmo_coef.shape[0]
    in_domain = jnp.arange(DB)[None, :] < block_count[:, None]
    onehot = ((domain[:, :, None] == jnp.arange(blocks)[None, None, :]) & in_domain[:, :, None]).astype(jnp.float32)
    tiles = lmo_coef.astype(jnp.float32).reshape(lmo_total, DB, BLK)
    dense_coef = jnp.einsum("ikb,ikn->bni", onehot, tiles, precision=lax.Precision.HIGHEST)
    return dense_coef.reshape(blocks * BLK, lmo_total).astype(jnp.bfloat16)


def select(half_ints, domain, block_count, blocks):
    row_total = half_ints.shape[0]
    lmo_total = half_ints.shape[2]
    in_domain = jnp.arange(PB)[None, :] < block_count[:, None]
    onehot = ((domain[:, :, None] == jnp.arange(blocks)[None, None, :]) & in_domain[:, :, None]).astype(jnp.float32)
    tiled = half_ints.reshape(row_total, blocks, BLK, lmo_total)
    picked = jnp.einsum("pbni,ikb->ipkn", tiled, onehot, precision=lax.Precision.HIGHEST)
    return picked.reshape(lmo_total, row_total, PB * BLK).astype(jnp.bfloat16)


def reference(aux_ints, lmo_coef, ao_domain, ao_count, pao_domain, pao_count, owner_order, pao_coef):
    blocks = aux_ints.shape[1] // BLK
    dense_coef = place(lmo_coef, ao_domain, ao_count, blocks)

    def transform(block_ints):
        row_total = block_ints.shape[0]
        half_ints = jnp.dot(block_ints.reshape(row_total * AO, AO), dense_coef,
                            preferred_element_type=jnp.float32).reshape(row_total, AO, -1)
        return select(half_ints, pao_domain, pao_count, blocks)

    stacked = lax.map(transform, aux_ints.reshape(NAUX // P_D, P_D, AO, AO))
    selected = jnp.transpose(stacked, (1, 0, 2, 3)).reshape(NLMO, NAUX, PB * BLK)
    ordered = selected[owner_order]

    def per_slot(operands):
        rows_here, coef_here = operands
        pair_row = jnp.dot(rows_here, coef_here, preferred_element_type=jnp.float32).astype(jnp.bfloat16)
        wide_row = pair_row.astype(jnp.float32)
        metric_row = jnp.dot(wide_row.T, wide_row, precision=lax.Precision.HIGHEST) / NAUX
        return pair_row, metric_row

    pair_ints, pair_metric = lax.map(per_slot, (ordered, pao_coef))
    return pair_ints, pair_metric
```

```python
import jax
import jax.numpy as jnp
from jax import lax
from jax.experimental import pallas as pl
from jax.experimental.pallas import tpu as pltpu
from jax.sharding import PartitionSpec as P

BLK = 128
DB = 3
PB = 3
USED = 8
AXES = ("aux", "lmo")


def half_kernel(
    owned, aux_ref, coef_ref, ao_dom_ref, ao_cnt_ref, pao_dom_ref, pao_cnt_ref, order_ref,
    send_ref, flat_ref, tiles_ref,
):
    sources, rows_each, _ = coef_ref.shape
    lmo_total = sources * rows_each
    row_total, ao_total, _ = aux_ref.shape
    blocks = ao_total // BLK
    cols = tiles_ref.shape[0]

    for src in range(sources):
        flat_ref[pl.ds(src * rows_each, rows_each), :] = coef_ref[src].astype(jnp.float32)
    coef_t = flat_ref[...].T

    ao_cnt = ao_cnt_ref[...]
    dense = []
    for b in range(blocks):
        total = jnp.zeros((BLK, lmo_total), jnp.float32)
        for k in range(DB):
            hit = (ao_dom_ref[k : k + 1, :] == b) & (ao_cnt > k)
            total = jnp.where(hit, coef_t[k * BLK : (k + 1) * BLK, :], total)
        dense.append(total)
    dense_t = jnp.concatenate(dense, axis=0).astype(jnp.bfloat16)

    code = pao_cnt_ref[...]
    for k in range(PB):
        code = code + pao_dom_ref[k : k + 1, :] * (4 * 8**k)
    code_col = jnp.broadcast_to(code, (8, lmo_total)).T[:, :1]
    cnt_col = code_col & 3
    lmo_id = lax.broadcasted_iota(jnp.int32, (lmo_total, lmo_total), 0)
    held = order_ref[...] == lmo_id
    cnt_slot = jnp.sum(jnp.where(held, cnt_col, 0), axis=0, keepdims=True)
    slot_id = lax.broadcasted_iota(jnp.int32, (1, lmo_total), 1)
    member = slot_id % owned
    first = (slot_id // owned) * USED
    for step in range(1, owned):
        first = first + jnp.where(member >= step, pltpu.roll(cnt_slot, step, 1), 0)
    first_col = jnp.sum(
        jnp.where(held, first, 0).astype(jnp.float32), axis=1, keepdims=True
    ).astype(jnp.int32)

    col_id = lax.broadcasted_iota(jnp.int32, (lmo_total, cols), 1)
    spread = jnp.zeros((lmo_total, cols), jnp.bool_)
    wanted = jnp.zeros((lmo_total, cols), jnp.int32)
    for k in range(PB):
        here = (col_id == first_col + k) & (cnt_col > k)
        wanted = jnp.where(here, (code_col >> (2 + 3 * k)) & 7, wanted)
        spread = spread | here
    block_row = jnp.sum(wanted, axis=0, keepdims=True)
    spread = jnp.where(spread, 1.0, 0.0).astype(jnp.bfloat16)
    weights = jnp.dot(dense_t, spread, preferred_element_type=jnp.float32).astype(jnp.bfloat16)

    for p in range(row_total):
        half = jnp.dot(aux_ref[p], weights, preferred_element_type=jnp.float32)
        picked = half[:BLK]
        for b in range(1, blocks):
            picked = jnp.where(block_row == b, half[b * BLK : (b + 1) * BLK], picked)
        tiles_ref[:, p, :] = picked.T
    for col in range(cols):
        dev, slot = divmod(col, USED)
        send_ref[dev, :, slot * BLK : (slot + 1) * BLK] = tiles_ref[col].astype(jnp.bfloat16)


def pair_kernel(owned, aux_total, me_ref, order_ref, cnt_ref, rows_ref, coef_ref, pair_ref, metric_ref):
    slot = 0
    for r in range(owned):
        count = cnt_ref[order_ref[me_ref[0] * owned + r]]
        parts = []
        for k in range(PB):
            at = pl.multiple_of(jnp.minimum(slot + k, USED - 1) * BLK, BLK)
            part = rows_ref[:, pl.ds(at, BLK)]
            parts.append(jnp.where(count > k, part, jnp.zeros_like(part)))
        slot = slot + count
        rows = jnp.concatenate(parts, axis=1)
        pair = jnp.dot(rows, coef_ref[r], preferred_element_type=jnp.float32).astype(jnp.bfloat16)
        pair_ref[r] = pair
        metric = lax.dot_general(
            pair, pair, (((0,), (0,)), ((), ())), preferred_element_type=jnp.float32
        )
        metric_ref[r] = metric / aux_total


def shards(aux_ints, lmo_coef, ao_domain, ao_count, pao_domain, pao_count, owner_order, pao_coef):
    devices = lax.axis_size(AXES)
    rows_each = lmo_coef.shape[0]
    lmo_total = devices * rows_each
    row_total, ao_total, _ = aux_ints.shape
    owned = pao_coef.shape[0]
    aux_total = devices * row_total
    cols = devices * USED

    coef = lax.all_to_all(
        jnp.broadcast_to(lmo_coef[None], (devices,) + lmo_coef.shape), AXES, split_axis=0, concat_axis=0, tiled=True
    )
    vmem = pl.BlockSpec(memory_space=pltpu.VMEM)
    smem = pl.BlockSpec(memory_space=pltpu.SMEM)
    send = pl.pallas_call(
        lambda *refs: half_kernel(owned, *refs),
        out_shape=jax.ShapeDtypeStruct((devices, row_total, USED * BLK), jnp.bfloat16),
        in_specs=[vmem] * 7,
        out_specs=vmem,
        scratch_shapes=[
            pltpu.VMEM((lmo_total, DB * BLK), jnp.float32),
            pltpu.VMEM((cols, row_total, BLK), jnp.float32),
        ],
        compiler_params=pltpu.CompilerParams(vmem_limit_bytes=60 * 2**20),
        cost_estimate=pl.CostEstimate(
            flops=2 * row_total * ao_total * ao_total * cols, bytes_accessed=2 * aux_ints.size, transcendentals=0
        ),
        name="half_transform",
    )(
        aux_ints, coef, ao_domain.T, ao_count[None], pao_domain.T, pao_count[None], owner_order[None]
    )
    received = lax.all_to_all(send, AXES, split_axis=0, concat_axis=0, tiled=True)
    return pl.pallas_call(
        lambda *refs: pair_kernel(owned, aux_total, *refs),
        out_shape=(
            jax.ShapeDtypeStruct((owned, aux_total, pao_coef.shape[2]), jnp.bfloat16),
            jax.ShapeDtypeStruct((owned, pao_coef.shape[2], pao_coef.shape[2]), jnp.float32),
        ),
        in_specs=[smem] * 3 + [vmem] * 2,
        out_specs=(vmem, vmem),
        name="pair_transform",
    )(
        lax.axis_index(AXES)[None].astype(jnp.int32), owner_order, pao_count,
        received.reshape(aux_total, USED * BLK), pao_coef,
    )


def solution(mesh):
    placed = (
        P(AXES, None, None),
        P(AXES, None),
        P(),
        P(),
        P(),
        P(),
        P(),
        P(AXES, None, None),
    )
    return jax.shard_map(
        shards,
        mesh=mesh,
        in_specs=placed,
        out_specs=(P(AXES, None, None), P(AXES, None, None)),
        check_vma=False,
    )
```

```python
import jax
import jax.numpy as jnp
from jax import lax
from jax.experimental import pallas as pl
from jax.experimental.pallas import tpu as pltpu
from jax.sharding import PartitionSpec as P

BLK = 128
DB = 3
PB = 3
USED = 8
AXES = ("aux", "lmo")


def prep_kernel(
    owned, used, coef_hbm, ao_dom_hbm, ao_cnt_hbm, pao_dom_hbm, pao_cnt_hbm, order_hbm,
    bcast_ref, spread_ref, table_ref,
    coef_ref, ao_dom_ref, ao_cnt_ref, pao_dom_ref, pao_cnt_ref, order_ref, sems,
):
    copies = [
        pltpu.make_async_copy(src, dst, sems.at[n])
        for n, (src, dst) in enumerate((
            (coef_hbm, coef_ref), (ao_dom_hbm, ao_dom_ref), (ao_cnt_hbm, ao_cnt_ref),
            (pao_dom_hbm, pao_dom_ref), (pao_cnt_hbm, pao_cnt_ref), (order_hbm, order_ref),
        ))
    ]
    for copy in copies:
        copy.start()
    for copy in copies:
        copy.wait()
    devices = bcast_ref.shape[0]
    lmo_total, cols = spread_ref.shape
    own = coef_ref[...]
    for dev in range(devices):
        bcast_ref[dev] = own

    code = pao_cnt_ref[...]
    for k in range(PB):
        code = code + pao_dom_ref[k : k + 1, :] * (4 * 8**k)
    code_col = jnp.broadcast_to(code, (8, lmo_total)).T[:, :1]
    cnt_col = code_col & 3
    lmo_id = lax.broadcasted_iota(jnp.int32, (lmo_total, lmo_total), 0)
    held = order_ref[...] == lmo_id
    cnt_slot = jnp.sum(jnp.where(held, cnt_col, 0), axis=0, keepdims=True)
    slot_id = lax.broadcasted_iota(jnp.int32, (1, lmo_total), 1)
    member = slot_id % owned
    first = (slot_id // owned) * used
    for step in range(1, owned):
        first = first + jnp.where(member >= step, pltpu.roll(cnt_slot, step, 1), 0)
    first_col = jnp.sum(
        jnp.where(held, first, 0).astype(jnp.float32), axis=1, keepdims=True
    ).astype(jnp.int32)

    col_id = lax.broadcasted_iota(jnp.int32, (lmo_total, cols), 1)
    spread = jnp.zeros((lmo_total, cols), jnp.bool_)
    wanted = jnp.zeros((lmo_total, cols), jnp.int32)
    for k in range(PB):
        here = (col_id == first_col + k) & (cnt_col > k)
        wanted = jnp.where(here, (code_col >> (2 + 3 * k)) & 7, wanted)
        spread = spread | here
    spread_ref[...] = jnp.where(spread, 1.0, 0.0).astype(jnp.bfloat16)
    table_ref[0:1, :] = jnp.sum(wanted, axis=0, keepdims=True)
    for k in range(DB):
        block = jnp.where(ao_cnt_ref[...] > k, ao_dom_ref[k : k + 1, :], -1)
        table_ref[1 + k : 2 + k, :lmo_total] = block


def half_kernel(aux_ref, coef_ref, spread_ref, table_ref, send_ref, flat_ref, tiles_ref):
    sources, rows_each, _ = coef_ref.shape
    lmo_total, cols = spread_ref.shape
    devices, row_total, width = send_ref.shape
    used = width // BLK
    blocks = aux_ref.shape[1] // BLK

    for src in range(sources):
        flat_ref[pl.ds(src * rows_each, rows_each), :] = coef_ref[src].astype(jnp.float32)
    coef_t = flat_ref[...].T
    dense = []
    for b in range(blocks):
        total = jnp.zeros((BLK, lmo_total), jnp.float32)
        for k in range(DB):
            hit = table_ref[1 + k : 2 + k, :lmo_total] == b
            total = jnp.where(hit, coef_t[k * BLK : (k + 1) * BLK, :], total)
        dense.append(total)
    dense_t = jnp.concatenate(dense, axis=0).astype(jnp.bfloat16)
    weights = jnp.dot(
        dense_t, spread_ref[...], preferred_element_type=jnp.float32
    ).astype(jnp.bfloat16)

    block_row = table_ref[0:1, :]
    for p in range(row_total):
        half = jnp.dot(aux_ref[p], weights, preferred_element_type=jnp.float32)
        picked = half[:BLK]
        for b in range(1, blocks):
            picked = jnp.where(block_row == b, half[b * BLK : (b + 1) * BLK], picked)
        tiles_ref[:, p, :] = picked.T
    for col in range(cols):
        dev, slot = divmod(col, used)
        send_ref[dev, :, slot * BLK : (slot + 1) * BLK] = tiles_ref[col].astype(jnp.bfloat16)


def pair_kernel(owned, aux_total, me_ref, order_ref, cnt_ref, rows_ref, coef_ref, pair_ref, metric_ref):
    slot = 0
    for r in range(owned):
        count = cnt_ref[order_ref[me_ref[0] * owned + r]]
        parts = []
        for k in range(PB):
            at = pl.multiple_of(jnp.minimum(slot + k, USED - 1) * BLK, BLK)
            part = rows_ref[:, pl.ds(at, BLK)]
            parts.append(jnp.where(count > k, part, jnp.zeros_like(part)))
        slot = slot + count
        rows = jnp.concatenate(parts, axis=1)
        pair = jnp.dot(rows, coef_ref[r], preferred_element_type=jnp.float32).astype(jnp.bfloat16)
        pair_ref[r] = pair
        metric = lax.dot_general(
            pair, pair, (((0,), (0,)), ((), ())), preferred_element_type=jnp.float32
        )
        metric_ref[r] = metric / aux_total


def shards(aux_ints, lmo_coef, ao_domain, ao_count, pao_domain, pao_count, owner_order, pao_coef):
    devices = lax.axis_size(AXES)
    rows_each = lmo_coef.shape[0]
    lmo_total = devices * rows_each
    row_total, ao_total, _ = aux_ints.shape
    owned = pao_coef.shape[0]
    aux_total = devices * row_total
    cols = devices * USED

    vmem = pl.BlockSpec(memory_space=pltpu.VMEM)
    smem = pl.BlockSpec(memory_space=pltpu.SMEM)
    small = pltpu.CompilerParams(vmem_limit_bytes=16 * 2**20)
    bcast, spread, table = pl.pallas_call(
        lambda *refs: prep_kernel(owned, USED, *refs),
        out_shape=(
            jax.ShapeDtypeStruct((devices,) + lmo_coef.shape, jnp.bfloat16),
            jax.ShapeDtypeStruct((lmo_total, cols), jnp.bfloat16),
            jax.ShapeDtypeStruct((8, cols), jnp.int32),
        ),
        in_specs=[pl.BlockSpec(memory_space=pltpu.HBM)] * 6,
        out_specs=(vmem,) * 3,
        scratch_shapes=[
            pltpu.VMEM(lmo_coef.shape, jnp.bfloat16),
            pltpu.VMEM((DB, lmo_total), jnp.int32),
            pltpu.VMEM((1, lmo_total), jnp.int32),
            pltpu.VMEM((PB, lmo_total), jnp.int32),
            pltpu.VMEM((1, lmo_total), jnp.int32),
            pltpu.VMEM((1, lmo_total), jnp.int32),
            pltpu.SemaphoreType.DMA((6,)),
        ],
        compiler_params=small,
        cost_estimate=pl.CostEstimate(flops=2 * 10**10, bytes_accessed=2**18, transcendentals=0),
        name="prep",
    )(*(
        pltpu.with_memory_space_constraint(x, pltpu.HBM)
        for x in (lmo_coef, ao_domain.T, ao_count[None], pao_domain.T, pao_count[None], owner_order[None])
    ))
    coef = lax.all_to_all(bcast, AXES, split_axis=0, concat_axis=0, tiled=True)
    send = pl.pallas_call(
        half_kernel,
        out_shape=jax.ShapeDtypeStruct((devices, row_total, USED * BLK), jnp.bfloat16),
        in_specs=[vmem] * 4,
        out_specs=vmem,
        scratch_shapes=[
            pltpu.VMEM((lmo_total, DB * BLK), jnp.float32),
            pltpu.VMEM((cols, row_total, BLK), jnp.float32),
        ],
        compiler_params=pltpu.CompilerParams(vmem_limit_bytes=24 * 2**20),
        cost_estimate=pl.CostEstimate(
            flops=2 * row_total * ao_total * ao_total * cols, bytes_accessed=2 * aux_ints.size, transcendentals=0
        ),
        name="half_transform",
    )(aux_ints, coef, spread, table)
    received = lax.all_to_all(send, AXES, split_axis=0, concat_axis=0, tiled=True)
    return pl.pallas_call(
        lambda *refs: pair_kernel(owned, aux_total, *refs),
        out_shape=(
            jax.ShapeDtypeStruct((owned, aux_total, pao_coef.shape[2]), jnp.bfloat16),
            jax.ShapeDtypeStruct((owned, pao_coef.shape[2], pao_coef.shape[2]), jnp.float32),
        ),
        in_specs=[smem] * 3 + [vmem] * 2,
        out_specs=(vmem, vmem),
        compiler_params=small,
        name="pair_transform",
    )(
        lax.axis_index(AXES)[None].astype(jnp.int32), owner_order, pao_count,
        received.reshape(aux_total, USED * BLK), pao_coef,
    )


def solution(mesh):
    placed = (
        P(AXES, None, None),
        P(AXES, None),
        P(),
        P(),
        P(),
        P(),
        P(),
        P(AXES, None, None),
    )
    return jax.shard_map(
        shards,
        mesh=mesh,
        in_specs=placed,
        out_specs=(P(AXES, None, None), P(AXES, None, None)),
        check_vma=False,
    )
```

```python
import jax
import jax.numpy as jnp
from jax import lax
from jax.experimental import pallas as pl
from jax.experimental.pallas import tpu as pltpu
from jax.sharding import PartitionSpec as P

BLK = 128
DB = 3
PB = 3
USED = 8
AXES = ("aux", "lmo")


def prep_kernel(
    owned, used, coef_hbm, ao_dom_hbm, ao_cnt_hbm, pao_dom_hbm, pao_cnt_hbm, order_hbm,
    bcast_ref, spread_ref, table_ref, counts_ref,
    coef_ref, ao_dom_ref, ao_cnt_ref, pao_dom_ref, pao_cnt_ref, order_ref, sems,
):
    copies = [
        pltpu.make_async_copy(src, dst, sems.at[n])
        for n, (src, dst) in enumerate((
            (coef_hbm, coef_ref), (ao_dom_hbm, ao_dom_ref), (ao_cnt_hbm, ao_cnt_ref),
            (pao_dom_hbm, pao_dom_ref), (pao_cnt_hbm, pao_cnt_ref), (order_hbm, order_ref),
        ))
    ]
    for copy in copies:
        copy.start()
    for copy in copies:
        copy.wait()
    devices = bcast_ref.shape[0]
    lmo_total, cols = spread_ref.shape
    own = coef_ref[...]
    for dev in range(devices):
        bcast_ref[dev] = own

    code = pao_cnt_ref[...]
    for k in range(PB):
        code = code + pao_dom_ref[k : k + 1, :] * (4 * 8**k)
    code_col = jnp.broadcast_to(code, (8, lmo_total)).T[:, :1]
    cnt_col = code_col & 3
    lmo_id = lax.broadcasted_iota(jnp.int32, (lmo_total, lmo_total), 0)
    held = order_ref[...] == lmo_id
    cnt_slot = jnp.sum(jnp.where(held, cnt_col, 0), axis=0, keepdims=True)
    slot_id = lax.broadcasted_iota(jnp.int32, (1, lmo_total), 1)
    member = slot_id % owned
    first = (slot_id // owned) * used
    for step in range(1, owned):
        first = first + jnp.where(member >= step, pltpu.roll(cnt_slot, step, 1), 0)
    first_col = jnp.sum(
        jnp.where(held, first, 0).astype(jnp.float32), axis=1, keepdims=True
    ).astype(jnp.int32)

    col_id = lax.broadcasted_iota(jnp.int32, (lmo_total, cols), 1)
    spread = jnp.zeros((lmo_total, cols), jnp.bool_)
    wanted = jnp.zeros((lmo_total, cols), jnp.int32)
    for k in range(PB):
        here = (col_id == first_col + k) & (cnt_col > k)
        wanted = jnp.where(here, (code_col >> (2 + 3 * k)) & 7, wanted)
        spread = spread | here
    spread_ref[...] = jnp.where(spread, 1.0, 0.0).astype(jnp.bfloat16)
    table_ref[0:1, :] = jnp.sum(wanted, axis=0, keepdims=True)
    for k in range(DB):
        block = jnp.where(ao_cnt_ref[...] > k, ao_dom_ref[k : k + 1, :], -1)
        table_ref[1 + k : 2 + k, :lmo_total] = block
    mine = lax.axis_index(AXES) * owned
    for r in range(owned):
        here = jnp.where(slot_id == mine + r, cnt_slot, 0)
        count = jnp.sum(here.astype(jnp.float32), axis=1, keepdims=True)
        counts_ref[r : r + 1, :] = jnp.broadcast_to(count, (1, 128)).astype(jnp.int32)


def half_kernel(aux_ref, coef_ref, spread_ref, table_ref, send_ref, flat_ref, tiles_ref):
    sources, rows_each, _ = coef_ref.shape
    lmo_total, cols = spread_ref.shape
    devices, row_total, width = send_ref.shape
    used = width // BLK
    blocks = aux_ref.shape[1] // BLK

    for src in range(sources):
        flat_ref[pl.ds(src * rows_each, rows_each), :] = coef_ref[src].astype(jnp.float32)
    coef_t = flat_ref[...].T
    dense = []
    for b in range(blocks):
        total = jnp.zeros((BLK, lmo_total), jnp.float32)
        for k in range(DB):
            hit = table_ref[1 + k : 2 + k, :lmo_total] == b
            total = jnp.where(hit, coef_t[k * BLK : (k + 1) * BLK, :], total)
        dense.append(total)
    dense_t = jnp.concatenate(dense, axis=0).astype(jnp.bfloat16)
    weights = jnp.dot(
        dense_t, spread_ref[...], preferred_element_type=jnp.float32
    ).astype(jnp.bfloat16)

    block_row = table_ref[0:1, :]
    for p in range(row_total):
        half = jnp.dot(aux_ref[p], weights, preferred_element_type=jnp.float32)
        picked = half[:BLK]
        for b in range(1, blocks):
            picked = jnp.where(block_row == b, half[b * BLK : (b + 1) * BLK], picked)
        tiles_ref[:, p, :] = picked.T
    for col in range(cols):
        dev, slot = divmod(col, used)
        send_ref[dev, :, slot * BLK : (slot + 1) * BLK] = tiles_ref[col].astype(jnp.bfloat16)


def pair_kernel(counts_ref, rows_ref, coef_ref, pair_hbm, metric_hbm, pair_ref, metric_ref, sems):
    owned, aux_total, _ = pair_ref.shape
    used = rows_ref.shape[1] // BLK
    counts = [counts_ref[r : r + 1, :][0, 0] for r in range(owned)]
    copies = []
    slot = 0
    for r in range(owned):
        parts = []
        for k in range(PB):
            at = pl.multiple_of(jnp.minimum(slot + k, used - 1) * BLK, BLK)
            part = rows_ref[:, pl.ds(at, BLK)]
            parts.append(jnp.where(counts[r] > k, part, jnp.zeros_like(part)))
        slot = slot + counts[r]
        rows = jnp.concatenate(parts, axis=1)
        pair = jnp.dot(rows, coef_ref[r], preferred_element_type=jnp.float32).astype(jnp.bfloat16)
        pair_ref[r] = pair
        copies.append(pltpu.make_async_copy(pair_ref.at[r], pair_hbm.at[r], sems.at[0, r]))
        copies[-1].start()
        metric = lax.dot_general(
            pair, pair, (((0,), (0,)), ((), ())), preferred_element_type=jnp.float32
        )
        metric_ref[r] = metric / aux_total
        copies.append(pltpu.make_async_copy(metric_ref.at[r], metric_hbm.at[r], sems.at[1, r]))
        copies[-1].start()
    for copy in copies:
        copy.wait()


def shards(aux_ints, lmo_coef, ao_domain, ao_count, pao_domain, pao_count, owner_order, pao_coef):
    devices = lax.axis_size(AXES)
    rows_each = lmo_coef.shape[0]
    lmo_total = devices * rows_each
    row_total, ao_total, _ = aux_ints.shape
    owned = pao_coef.shape[0]
    aux_total = devices * row_total
    cols = devices * USED

    vmem = pl.BlockSpec(memory_space=pltpu.VMEM)
    small = pltpu.CompilerParams(vmem_limit_bytes=16 * 2**20)
    bcast, spread, table, counts = pl.pallas_call(
        lambda *refs: prep_kernel(owned, USED, *refs),
        out_shape=(
            jax.ShapeDtypeStruct((devices,) + lmo_coef.shape, jnp.bfloat16),
            jax.ShapeDtypeStruct((lmo_total, cols), jnp.bfloat16),
            jax.ShapeDtypeStruct((8, cols), jnp.int32),
            jax.ShapeDtypeStruct((owned, 128), jnp.int32),
        ),
        in_specs=[pl.BlockSpec(memory_space=pltpu.HBM)] * 6,
        out_specs=(vmem,) * 4,
        scratch_shapes=[
            pltpu.VMEM(lmo_coef.shape, jnp.bfloat16),
            pltpu.VMEM((DB, lmo_total), jnp.int32),
            pltpu.VMEM((1, lmo_total), jnp.int32),
            pltpu.VMEM((PB, lmo_total), jnp.int32),
            pltpu.VMEM((1, lmo_total), jnp.int32),
            pltpu.VMEM((1, lmo_total), jnp.int32),
            pltpu.SemaphoreType.DMA((6,)),
        ],
        compiler_params=small,
        cost_estimate=pl.CostEstimate(flops=2 * 10**10, bytes_accessed=2**18, transcendentals=0),
        name="prep",
    )(*(
        pltpu.with_memory_space_constraint(x, pltpu.HBM)
        for x in (lmo_coef, ao_domain.T, ao_count[None], pao_domain.T, pao_count[None], owner_order[None])
    ))
    coef = lax.all_to_all(bcast, AXES, split_axis=0, concat_axis=0, tiled=True)
    send = pl.pallas_call(
        half_kernel,
        out_shape=jax.ShapeDtypeStruct((devices, row_total, USED * BLK), jnp.bfloat16),
        in_specs=[vmem] * 4,
        out_specs=vmem,
        scratch_shapes=[
            pltpu.VMEM((lmo_total, DB * BLK), jnp.float32),
            pltpu.VMEM((cols, row_total, BLK), jnp.float32),
        ],
        compiler_params=pltpu.CompilerParams(vmem_limit_bytes=24 * 2**20),
        cost_estimate=pl.CostEstimate(
            flops=2 * row_total * ao_total * ao_total * cols, bytes_accessed=2 * aux_ints.size, transcendentals=0
        ),
        name="half_transform",
    )(aux_ints, coef, spread, table)
    received = lax.all_to_all(send, AXES, split_axis=0, concat_axis=0, tiled=True)
    outs = (
        ((owned, aux_total, pao_coef.shape[2]), jnp.bfloat16),
        ((owned, pao_coef.shape[2], pao_coef.shape[2]), jnp.float32),
    )
    return pl.pallas_call(
        pair_kernel,
        out_shape=tuple(jax.ShapeDtypeStruct(*out) for out in outs),
        in_specs=[vmem] * 3,
        out_specs=(pl.BlockSpec(memory_space=pltpu.HBM),) * 2,
        scratch_shapes=[pltpu.VMEM(*out) for out in outs] + [pltpu.SemaphoreType.DMA((2, owned))],
        compiler_params=small,
        name="pair_transform",
    )(counts, received.reshape(aux_total, USED * BLK), pao_coef)


def solution(mesh):
    placed = (
        P(AXES, None, None),
        P(AXES, None),
        P(),
        P(),
        P(),
        P(),
        P(),
        P(AXES, None, None),
    )
    return jax.shard_map(
        shards,
        mesh=mesh,
        in_specs=placed,
        out_specs=(P(AXES, None, None), P(AXES, None, None)),
        check_vma=False,
    )
```

```python
import jax
import jax.numpy as jnp
from jax import lax
from jax.experimental import pallas as pl
from jax.experimental.pallas import tpu as pltpu
from jax.sharding import PartitionSpec as P

BLK = 128
DB = 3
PB = 3
USED = 8
AXES = ("aux", "lmo")

GATHER_ORDER = (
    10, 17, 31, 9, 5, 30, 29, 28, 24, 4, 15, 16, 18, 8, 25, 1, 0, 12, 6, 2, 3, 14, 13, 27, 22,
    23, 19, 20, 11, 21, 26, 7,
)
SEND_ORDER = (
    24, 27, 5, 30, 1, 19, 25, 2, 12, 18, 14, 6, 7, 9, 22, 8, 4, 11, 3, 20, 0, 21, 10, 29, 26,
    16, 28, 23, 31, 13, 17, 15,
)


def participants(order, devices):
    rank = {device: place for place, device in enumerate(order)}
    return sorted(range(devices), key=lambda device: (rank[device % len(order)], device))


def exchange(blocks, order):
    return lax.all_to_all(
        blocks, AXES, split_axis=0, concat_axis=0, tiled=True, axis_index_groups=[order]
    )


def prep_kernel(
    owned, used, coef_hbm, ao_dom_hbm, ao_cnt_hbm, pao_dom_hbm, pao_cnt_hbm, order_hbm,
    bcast_ref, spread_ref, table_ref, counts_ref,
    coef_ref, ao_dom_ref, ao_cnt_ref, pao_dom_ref, pao_cnt_ref, order_ref, sems,
):
    copies = [
        pltpu.make_async_copy(src, dst, sems.at[n])
        for n, (src, dst) in enumerate((
            (coef_hbm, coef_ref), (ao_dom_hbm, ao_dom_ref), (ao_cnt_hbm, ao_cnt_ref),
            (pao_dom_hbm, pao_dom_ref), (pao_cnt_hbm, pao_cnt_ref), (order_hbm, order_ref),
        ))
    ]
    for copy in copies:
        copy.start()
    for copy in copies:
        copy.wait()
    devices = bcast_ref.shape[0]
    lmo_total, cols = spread_ref.shape
    own = coef_ref[...]
    for dev in range(devices):
        bcast_ref[dev] = own

    code = pao_cnt_ref[...]
    for k in range(PB):
        code = code + pao_dom_ref[k : k + 1, :] * (4 * 8**k)
    code_col = jnp.broadcast_to(code, (8, lmo_total)).T[:, :1]
    cnt_col = code_col & 3
    lmo_id = lax.broadcasted_iota(jnp.int32, (lmo_total, lmo_total), 0)
    held = order_ref[...] == lmo_id
    cnt_slot = jnp.sum(jnp.where(held, cnt_col, 0), axis=0, keepdims=True)
    slot_id = lax.broadcasted_iota(jnp.int32, (1, lmo_total), 1)
    member = slot_id % owned
    first = (slot_id // owned) * used
    for step in range(1, owned):
        first = first + jnp.where(member >= step, pltpu.roll(cnt_slot, step, 1), 0)
    first_col = jnp.sum(
        jnp.where(held, first, 0).astype(jnp.float32), axis=1, keepdims=True
    ).astype(jnp.int32)

    col_id = lax.broadcasted_iota(jnp.int32, (lmo_total, cols), 1)
    spread = jnp.zeros((lmo_total, cols), jnp.bool_)
    wanted = jnp.zeros((lmo_total, cols), jnp.int32)
    for k in range(PB):
        here = (col_id == first_col + k) & (cnt_col > k)
        wanted = jnp.where(here, (code_col >> (2 + 3 * k)) & 7, wanted)
        spread = spread | here
    spread_ref[...] = jnp.where(spread, 1.0, 0.0).astype(jnp.bfloat16)
    table_ref[0:1, :] = jnp.sum(wanted, axis=0, keepdims=True)
    for k in range(DB):
        block = jnp.where(ao_cnt_ref[...] > k, ao_dom_ref[k : k + 1, :], -1)
        table_ref[1 + k : 2 + k, :lmo_total] = block
    mine = lax.axis_index(AXES) * owned
    for r in range(owned):
        here = jnp.where(slot_id == mine + r, cnt_slot, 0)
        count = jnp.sum(here.astype(jnp.float32), axis=1, keepdims=True)
        counts_ref[r : r + 1, :] = jnp.broadcast_to(count, (1, 128)).astype(jnp.int32)


def half_kernel(gather_order, send_order, aux_ref, coef_ref, spread_ref, table_ref, send_ref, flat_ref, tiles_ref):
    rows_each = coef_ref.shape[1]
    lmo_total, cols = spread_ref.shape
    devices, row_total, width = send_ref.shape
    used = width // BLK
    blocks = aux_ref.shape[1] // BLK

    for place, src in enumerate(gather_order):
        flat_ref[pl.ds(src * rows_each, rows_each), :] = coef_ref[place].astype(jnp.float32)
    coef_t = flat_ref[...].T
    dense = []
    for b in range(blocks):
        total = jnp.zeros((BLK, lmo_total), jnp.float32)
        for k in range(DB):
            hit = table_ref[1 + k : 2 + k, :lmo_total] == b
            total = jnp.where(hit, coef_t[k * BLK : (k + 1) * BLK, :], total)
        dense.append(total)
    dense_t = jnp.concatenate(dense, axis=0).astype(jnp.bfloat16)
    weights = jnp.dot(
        dense_t, spread_ref[...], preferred_element_type=jnp.float32
    ).astype(jnp.bfloat16)

    block_row = table_ref[0:1, :]
    for p in range(row_total):
        half = jnp.dot(aux_ref[p], weights, preferred_element_type=jnp.float32)
        picked = half[:BLK]
        for b in range(1, blocks):
            picked = jnp.where(block_row == b, half[b * BLK : (b + 1) * BLK], picked)
        tiles_ref[pl.ds(p, cols, stride=row_total), :] = picked.T
    for place, dev in enumerate(send_order):
        for slot in range(used):
            tile = tiles_ref[pl.ds((dev * used + slot) * row_total, row_total), :]
            send_ref[place, :, slot * BLK : (slot + 1) * BLK] = tile.astype(jnp.bfloat16)


def pair_kernel(send_order, counts_ref, rows_ref, coef_ref, pair_hbm, metric_hbm, pair_ref, metric_ref, sems):
    owned, aux_total, _ = pair_ref.shape
    used = rows_ref.shape[1] // BLK
    row_total = aux_total // len(send_order)
    places = sorted(range(len(send_order)), key=lambda place: send_order[place])
    counts = [counts_ref[r : r + 1, :][0, 0] for r in range(owned)]
    slot = 0
    for r in range(owned):
        parts = []
        for k in range(PB):
            at = pl.multiple_of(jnp.minimum(slot + k, used - 1) * BLK, BLK)
            part = rows_ref[:, pl.ds(at, BLK)]
            parts.append(jnp.where(counts[r] > k, part, jnp.zeros_like(part)))
        slot = slot + counts[r]
        rows = jnp.concatenate(parts, axis=1)
        pair = jnp.dot(rows, coef_ref[r], preferred_element_type=jnp.float32)
        groups = [pair[place * row_total : (place + 1) * row_total] for place in places]
        pair_ref[r] = jnp.concatenate(groups, axis=0).astype(jnp.bfloat16)
    copies = [pltpu.make_async_copy(pair_ref, pair_hbm, sems.at[0])]
    copies[0].start()
    for r in range(owned):
        pair = pair_ref[r]
        metric = lax.dot_general(
            pair, pair, (((0,), (0,)), ((), ())), preferred_element_type=jnp.float32
        )
        metric_ref[r] = metric / aux_total
        if r % 1 == 0:
            some = pl.ds(r - 0, 1)
            copies.append(
                pltpu.make_async_copy(metric_ref.at[some], metric_hbm.at[some], sems.at[1 + r // 1])
            )
            copies[-1].start()
    for copy in copies:
        copy.wait()


def shards(aux_ints, lmo_coef, ao_domain, ao_count, pao_domain, pao_count, owner_order, pao_coef):
    devices = lax.axis_size(AXES)
    rows_each = lmo_coef.shape[0]
    lmo_total = devices * rows_each
    row_total, ao_total, _ = aux_ints.shape
    owned = pao_coef.shape[0]
    aux_total = devices * row_total
    cols = devices * USED

    vmem = pl.BlockSpec(memory_space=pltpu.VMEM)
    small = pltpu.CompilerParams(vmem_limit_bytes=16 * 2**20)
    bcast, spread, table, counts = pl.pallas_call(
        lambda *refs: prep_kernel(owned, USED, *refs),
        out_shape=(
            jax.ShapeDtypeStruct((devices,) + lmo_coef.shape, jnp.bfloat16),
            jax.ShapeDtypeStruct((lmo_total, cols), jnp.bfloat16),
            jax.ShapeDtypeStruct((8, cols), jnp.int32),
            jax.ShapeDtypeStruct((owned, 128), jnp.int32),
        ),
        in_specs=[pl.BlockSpec(memory_space=pltpu.HBM)] * 6,
        out_specs=(vmem,) * 4,
        scratch_shapes=[
            pltpu.VMEM(lmo_coef.shape, jnp.bfloat16),
            pltpu.VMEM((DB, lmo_total), jnp.int32),
            pltpu.VMEM((1, lmo_total), jnp.int32),
            pltpu.VMEM((PB, lmo_total), jnp.int32),
            pltpu.VMEM((1, lmo_total), jnp.int32),
            pltpu.VMEM((1, lmo_total), jnp.int32),
            pltpu.SemaphoreType.DMA((6,)),
        ],
        compiler_params=small,
        cost_estimate=pl.CostEstimate(flops=2 * 10**10, bytes_accessed=2**18, transcendentals=0),
        name="prep",
    )(*(
        pltpu.with_memory_space_constraint(x, pltpu.HBM)
        for x in (lmo_coef, ao_domain.T, ao_count[None], pao_domain.T, pao_count[None], owner_order[None])
    ))
    gather_order = participants(GATHER_ORDER, devices)
    send_order = participants(SEND_ORDER, devices)
    coef = exchange(bcast, gather_order)
    send = pl.pallas_call(
        lambda *refs: half_kernel(gather_order, send_order, *refs),
        out_shape=jax.ShapeDtypeStruct((devices, row_total, USED * BLK), jnp.bfloat16),
        in_specs=[vmem] * 4,
        out_specs=vmem,
        scratch_shapes=[
            pltpu.VMEM((lmo_total, DB * BLK), jnp.float32),
            pltpu.VMEM((cols * row_total, BLK), jnp.float32),
        ],
        compiler_params=pltpu.CompilerParams(vmem_limit_bytes=24 * 2**20),
        cost_estimate=pl.CostEstimate(
            flops=2 * row_total * ao_total * ao_total * cols, bytes_accessed=2 * aux_ints.size, transcendentals=0
        ),
        name="half_transform",
    )(aux_ints, coef, spread, table)
    received = exchange(send, send_order)
    outs = (
        ((owned, aux_total, pao_coef.shape[2]), jnp.bfloat16),
        ((owned, pao_coef.shape[2], pao_coef.shape[2]), jnp.float32),
    )
    return pl.pallas_call(
        lambda *refs: pair_kernel(send_order, *refs),
        out_shape=tuple(jax.ShapeDtypeStruct(*out) for out in outs),
        in_specs=[vmem] * 3,
        out_specs=(pl.BlockSpec(memory_space=pltpu.HBM),) * 2,
        scratch_shapes=[pltpu.VMEM(*out) for out in outs] + [pltpu.SemaphoreType.DMA((1 + owned // 1,))],
        compiler_params=small,
        name="pair_transform",
    )(counts, received.reshape(aux_total, USED * BLK), pao_coef)


def solution(mesh):
    placed = (
        P(AXES, None, None),
        P(AXES, None),
        P(),
        P(),
        P(),
        P(),
        P(),
        P(AXES, None, None),
    )
    return jax.shard_map(
        shards,
        mesh=mesh,
        in_specs=placed,
        out_specs=(P(AXES, None, None), P(AXES, None, None)),
        check_vma=False,
    )
```

```python
import jax
import jax.numpy as jnp
from jax import lax
from jax.experimental import pallas as pl
from jax.experimental.pallas import tpu as pltpu
from jax.sharding import PartitionSpec as P

BLK = 128
DB = 3
PB = 3
USED = 8
AXES = ("aux", "lmo")

GATHER_ORDER = (
    10, 17, 31, 9, 5, 30, 29, 28, 24, 4, 15, 16, 18, 8, 25, 1, 0, 12, 6, 2, 3, 14, 13, 27, 22,
    23, 19, 20, 11, 21, 26, 7,
)
SEND_ORDER = (
    24, 27, 5, 30, 1, 19, 25, 2, 12, 18, 14, 6, 7, 9, 22, 8, 4, 11, 3, 20, 0, 21, 10, 29, 26,
    16, 28, 23, 31, 13, 17, 15,
)


def participants(order, devices):
    rank = {device: place for place, device in enumerate(order)}
    return sorted(range(devices), key=lambda device: (rank[device % len(order)], device))


def exchange(blocks, order):
    return lax.all_to_all(
        blocks, AXES, split_axis=0, concat_axis=0, tiled=True, axis_index_groups=[order]
    )


def spread_kernel(coef_hbm, bcast_ref, coef_ref, sem):
    copy = pltpu.make_async_copy(coef_hbm, coef_ref, sem)
    copy.start()
    copy.wait()
    own = coef_ref[...]
    for dev in range(bcast_ref.shape[0]):
        bcast_ref[dev] = own


def rows_of(row, count):
    return jnp.broadcast_to(row, (count, row.shape[1])).astype(jnp.bfloat16)


def half_kernel(
    owned, gather_order, send_order,
    aux_ref, coef_ref, ao_dom_ref, ao_cnt_ref, pao_dom_ref, pao_cnt_ref, order_ref,
    send_ref, counts_ref, flat_ref, tiles_ref,
):
    rows_each = coef_ref.shape[1]
    lmo_total = order_ref.shape[1]
    devices, row_total, width = send_ref.shape
    used = width // BLK
    cols = devices * used
    blocks = aux_ref.shape[1] // BLK

    lmo_id = lax.broadcasted_iota(jnp.int32, (lmo_total, lmo_total), 0)
    held = jnp.where(order_ref[...] == lmo_id, 1.0, 0.0).astype(jnp.bfloat16)
    cnt_slot = jnp.dot(
        rows_of(pao_cnt_ref[...], 8), held, preferred_element_type=jnp.float32
    )[:1].astype(jnp.int32)
    slot_id = lax.broadcasted_iota(jnp.int32, (1, lmo_total), 1)
    member = slot_id % owned
    base = jnp.zeros_like(cnt_slot)
    for step in range(1, owned):
        base = base + jnp.where(member >= step, pltpu.roll(cnt_slot, step, 1), 0)
    facts = jnp.concatenate(
        [rows_of(fact, 128) for fact in (slot_id // owned, base, cnt_slot)], axis=0
    )
    facts = lax.dot_general(
        held, facts, (((1,), (1,)), ((), ())), preferred_element_type=jnp.float32
    ).astype(jnp.int32)
    first = facts[:, :128] * used + facts[:, 128:256]
    count = facts[:, 256:]

    lane = lax.broadcasted_iota(jnp.int32, (lmo_total, 128), 1)
    spread, block_row = [], []
    for part in range(cols // 128):
        hits = [
            jnp.where((first + k == lane + part * 128) & (count > k), 1.0, 0.0) for k in range(PB)
        ]
        spread.append(sum(hits).astype(jnp.bfloat16))
        block_row.append(
            sum(
                jnp.dot(
                    rows_of(pao_dom_ref[k : k + 1, :], 8),
                    hits[k].astype(jnp.bfloat16),
                    preferred_element_type=jnp.float32,
                )
                for k in range(PB)
            )[:1]
        )
    spread = jnp.concatenate(spread, axis=1)
    block_row = jnp.concatenate(block_row, axis=1)

    for place, src in enumerate(gather_order):
        flat_ref[pl.ds(src * rows_each, rows_each), :] = coef_ref[place].astype(jnp.float32)
    coef_t = flat_ref[...].T
    homes = [
        jnp.where(ao_cnt_ref[...] > k, ao_dom_ref[k : k + 1, :], -1) for k in range(DB)
    ]
    dense = []
    for b in range(blocks):
        total = jnp.zeros((BLK, lmo_total), jnp.float32)
        for k in range(DB):
            total = jnp.where(homes[k] == b, coef_t[k * BLK : (k + 1) * BLK, :], total)
        dense.append(total)
    dense_t = jnp.concatenate(dense, axis=0).astype(jnp.bfloat16)
    weights = jnp.dot(dense_t, spread, preferred_element_type=jnp.float32).astype(jnp.bfloat16)

    for p in range(row_total):
        half = jnp.dot(aux_ref[p], weights, preferred_element_type=jnp.float32)
        picked = half[:BLK]
        for b in range(1, blocks):
            picked = jnp.where(block_row == b, half[b * BLK : (b + 1) * BLK], picked)
        tiles_ref[pl.ds(p, cols, stride=row_total), :] = picked.T
    mine = lax.axis_index(AXES) * owned
    for r in range(owned):
        here = jnp.where(slot_id == mine + r, cnt_slot, 0).astype(jnp.float32)
        here = jnp.sum(here, axis=1, keepdims=True).astype(jnp.int32)
        counts_ref[r : r + 1, :] = jnp.broadcast_to(here, (1, 128))
    for place, dev in enumerate(send_order):
        for slot in range(used):
            tile = tiles_ref[pl.ds((dev * used + slot) * row_total, row_total), :]
            send_ref[place, :, slot * BLK : (slot + 1) * BLK] = tile.astype(jnp.bfloat16)


def pair_kernel(send_order, counts_ref, rows_ref, coef_ref, pair_hbm, metric_hbm, pair_ref, metric_ref, sems):
    owned, aux_total, _ = pair_ref.shape
    used = rows_ref.shape[1] // BLK
    row_total = aux_total // len(send_order)
    places = sorted(range(len(send_order)), key=lambda place: send_order[place])
    counts = [counts_ref[r : r + 1, :][0, 0] for r in range(owned)]
    copies = []
    slot = 0
    for r in range(owned):
        parts = []
        for k in range(PB):
            at = pl.multiple_of(jnp.minimum(slot + k, used - 1) * BLK, BLK)
            part = rows_ref[:, pl.ds(at, BLK)]
            parts.append(jnp.where(counts[r] > k, part, jnp.zeros_like(part)))
        slot = slot + counts[r]
        rows = jnp.concatenate(parts, axis=1)
        pair = jnp.dot(rows, coef_ref[r], preferred_element_type=jnp.float32)
        groups = [pair[place * row_total : (place + 1) * row_total] for place in places]
        pair_ref[r] = jnp.concatenate(groups, axis=0).astype(jnp.bfloat16)
        copies.append(pltpu.make_async_copy(pair_ref.at[r], pair_hbm.at[r], sems.at[owned + r]))
        copies[-1].start()
    for r in range(owned):
        pair = pair_ref[r]
        metric = lax.dot_general(
            pair, pair, (((0,), (0,)), ((), ())), preferred_element_type=jnp.float32
        )
        metric_ref[r] = metric / aux_total
        copies.append(pltpu.make_async_copy(metric_ref.at[r], metric_hbm.at[r], sems.at[r]))
        copies[-1].start()
    for copy in copies:
        copy.wait()


def shards(aux_ints, lmo_coef, ao_domain, ao_count, pao_domain, pao_count, owner_order, pao_coef):
    devices = lax.axis_size(AXES)
    rows_each = lmo_coef.shape[0]
    lmo_total = devices * rows_each
    row_total, ao_total, _ = aux_ints.shape
    owned = pao_coef.shape[0]
    aux_total = devices * row_total
    cols = devices * USED

    vmem = pl.BlockSpec(memory_space=pltpu.VMEM)
    small = pltpu.CompilerParams(vmem_limit_bytes=16 * 2**20)
    bcast = pl.pallas_call(
        spread_kernel,
        out_shape=jax.ShapeDtypeStruct((devices,) + lmo_coef.shape, jnp.bfloat16),
        in_specs=[pl.BlockSpec(memory_space=pltpu.HBM)],
        out_specs=vmem,
        scratch_shapes=[pltpu.VMEM(lmo_coef.shape, jnp.bfloat16), pltpu.SemaphoreType.DMA],
        compiler_params=small,
        cost_estimate=pl.CostEstimate(flops=2 * 10**10, bytes_accessed=2**18, transcendentals=0),
        name="spread",
    )(pltpu.with_memory_space_constraint(lmo_coef, pltpu.HBM))
    gather_order = participants(GATHER_ORDER, devices)
    send_order = participants(SEND_ORDER, devices)
    coef = exchange(bcast, gather_order)
    send, counts = pl.pallas_call(
        lambda *refs: half_kernel(owned, gather_order, send_order, *refs),
        out_shape=(
            jax.ShapeDtypeStruct((devices, row_total, USED * BLK), jnp.bfloat16),
            jax.ShapeDtypeStruct((owned, 128), jnp.int32),
        ),
        in_specs=[vmem] * 7,
        out_specs=(vmem,) * 2,
        scratch_shapes=[
            pltpu.VMEM((lmo_total, DB * BLK), jnp.float32),
            pltpu.VMEM((cols * row_total, BLK), jnp.float32),
        ],
        compiler_params=pltpu.CompilerParams(vmem_limit_bytes=24 * 2**20),
        cost_estimate=pl.CostEstimate(
            flops=2 * row_total * ao_total * ao_total * cols, bytes_accessed=2 * aux_ints.size, transcendentals=0
        ),
        name="half_transform",
    )(aux_ints, coef, ao_domain.T, ao_count[None], pao_domain.T, pao_count[None], owner_order[None])
    received = exchange(send, send_order)
    outs = (
        ((owned, aux_total, pao_coef.shape[2]), jnp.bfloat16),
        ((owned, pao_coef.shape[2], pao_coef.shape[2]), jnp.float32),
    )
    return pl.pallas_call(
        lambda *refs: pair_kernel(send_order, *refs),
        out_shape=tuple(jax.ShapeDtypeStruct(*out) for out in outs),
        in_specs=[vmem] * 3,
        out_specs=(pl.BlockSpec(memory_space=pltpu.HBM),) * 2,
        scratch_shapes=[pltpu.VMEM(*out) for out in outs] + [pltpu.SemaphoreType.DMA((2 * owned,))],
        compiler_params=small,
        name="pair_transform",
    )(counts, received.reshape(aux_total, USED * BLK), pao_coef)


def solution(mesh):
    placed = (
        P(AXES, None, None),
        P(AXES, None),
        P(),
        P(),
        P(),
        P(),
        P(),
        P(AXES, None, None),
    )
    return jax.shard_map(
        shards,
        mesh=mesh,
        in_specs=placed,
        out_specs=(P(AXES, None, None), P(AXES, None, None)),
        check_vma=False,
    )
```

```python
import jax
import jax.numpy as jnp
from jax import lax
from jax.experimental import pallas as pl
from jax.experimental.pallas import tpu as pltpu
from jax.sharding import PartitionSpec as P

BLK = 128
DB = 3
PB = 3
USED = 8
AXES = ("aux", "lmo")

GATHER_ORDER = (
    11, 0, 25, 21, 31, 22, 5, 20, 14, 30, 13, 16, 9, 7, 17, 1, 15, 12, 4, 2, 10, 3, 18, 19,
    27, 24, 29, 6, 8, 28, 26, 23,
)
SEND_ORDER = (
    24, 27, 5, 30, 1, 19, 25, 26, 16, 2, 12, 18, 14, 6, 7, 9, 22, 8, 4, 11, 3, 20, 0, 21, 10,
    29, 28, 23, 31, 13, 17, 15,
)


def participants(order, devices):
    rank = {device: place for place, device in enumerate(order)}
    return sorted(range(devices), key=lambda device: (rank[device % len(order)], device))


def exchange(blocks, order):
    return lax.all_to_all(
        blocks, AXES, split_axis=0, concat_axis=0, tiled=True, axis_index_groups=[order]
    )


def spread_kernel(coef_hbm, bcast_ref, coef_ref, sem):
    copy = pltpu.make_async_copy(coef_hbm, coef_ref, sem)
    copy.start()
    copy.wait()
    own = coef_ref[...]
    for dev in range(bcast_ref.shape[0]):
        bcast_ref[dev] = own


def rows_of(row, count):
    return jnp.broadcast_to(row, (count, row.shape[1])).astype(jnp.bfloat16)


def half_kernel(
    owned, gather_order, send_order,
    aux_ref, coef_ref, ao_dom_ref, ao_cnt_ref, pao_dom_ref, pao_cnt_ref, order_ref,
    send_ref, counts_ref, flat_ref, tiles_ref,
):
    rows_each = coef_ref.shape[1]
    lmo_total = order_ref.shape[1]
    devices, row_total, width = send_ref.shape
    used = width // BLK
    cols = devices * used
    blocks = aux_ref.shape[1] // BLK

    lmo_id = lax.broadcasted_iota(jnp.int32, (lmo_total, lmo_total), 0)
    held = jnp.where(order_ref[...] == lmo_id, 1.0, 0.0).astype(jnp.bfloat16)
    cnt_slot = jnp.dot(
        rows_of(pao_cnt_ref[...], 8), held, preferred_element_type=jnp.float32
    )[:1].astype(jnp.int32)
    slot_id = lax.broadcasted_iota(jnp.int32, (1, lmo_total), 1)
    member = slot_id % owned
    base = jnp.zeros_like(cnt_slot)
    for step in range(1, owned):
        base = base + jnp.where(member >= step, pltpu.roll(cnt_slot, step, 1), 0)
    facts = jnp.concatenate(
        [rows_of(fact, 128) for fact in (slot_id // owned, base, cnt_slot)], axis=0
    )
    facts = lax.dot_general(
        held, facts, (((1,), (1,)), ((), ())), preferred_element_type=jnp.float32
    ).astype(jnp.int32)
    first = facts[:, :128] * used + facts[:, 128:256]
    count = facts[:, 256:]

    lane = lax.broadcasted_iota(jnp.int32, (lmo_total, 128), 1)
    spread = []
    for part in range(cols // 128):
        place = lane + part * 128 - first
        spread.append(jnp.where((place >= 0) & (place < count), 1.0, 0.0))
    spread = jnp.concatenate(spread, axis=1).astype(jnp.bfloat16)

    by_lmo = lax.dot_general(
        jnp.concatenate([rows_of(fact, 16) for fact in (slot_id // owned, base)], axis=0),
        held, (((1,), (1,)), ((), ())), preferred_element_type=jnp.float32,
    ).astype(jnp.bfloat16)
    by_lmo = jnp.concatenate(
        [by_lmo] + [rows_of(pao_dom_ref[k : k + 1, :], 16) for k in range(PB)], axis=0
    )
    by_col = jnp.dot(by_lmo, spread, preferred_element_type=jnp.float32)
    by_col = [by_col[16 * n : 16 * n + 1] for n in range(2 + PB)]
    col_id = lax.broadcasted_iota(jnp.int32, (1, cols), 1).astype(jnp.float32)
    place = col_id - (by_col[0] * used + by_col[1])
    block_row = by_col[2]
    for k in range(1, PB):
        block_row = jnp.where(place >= k, by_col[2 + k], block_row)

    for place, src in enumerate(gather_order):
        flat_ref[pl.ds(src * rows_each, rows_each), :] = coef_ref[place].astype(jnp.float32)
    coef_t = flat_ref[...].T
    homes = [
        jnp.where(ao_cnt_ref[...] > k, ao_dom_ref[k : k + 1, :], -1) for k in range(DB)
    ]
    dense = []
    for b in range(blocks):
        total = jnp.zeros((BLK, lmo_total), jnp.float32)
        for k in range(DB):
            total = jnp.where(homes[k] == b, coef_t[k * BLK : (k + 1) * BLK, :], total)
        dense.append(total)
    dense_t = jnp.concatenate(dense, axis=0).astype(jnp.bfloat16)
    weights = jnp.dot(dense_t, spread, preferred_element_type=jnp.float32).astype(jnp.bfloat16)

    for p in range(row_total):
        half = jnp.dot(aux_ref[p], weights, preferred_element_type=jnp.float32)
        picked = half[:BLK]
        for b in range(1, blocks):
            picked = jnp.where(block_row == b, half[b * BLK : (b + 1) * BLK], picked)
        tiles_ref[pl.ds(p, cols, stride=row_total), :] = picked.T
    mine = lax.axis_index(AXES) * owned
    for r in range(owned):
        here = jnp.where(slot_id == mine + r, cnt_slot, 0).astype(jnp.float32)
        here = jnp.sum(here, axis=1, keepdims=True).astype(jnp.int32)
        counts_ref[r : r + 1, :] = jnp.broadcast_to(here, (1, 128))
    for place, dev in enumerate(send_order):
        for slot in range(used):
            tile = tiles_ref[pl.ds((dev * used + slot) * row_total, row_total), :]
            send_ref[place, :, slot * BLK : (slot + 1) * BLK] = tile.astype(jnp.bfloat16)


def pair_kernel(send_order, counts_ref, rows_ref, coef_ref, pair_hbm, metric_hbm, pair_ref, metric_ref, sems):
    owned, aux_total, _ = pair_ref.shape
    used = rows_ref.shape[1] // BLK
    row_total = aux_total // len(send_order)
    places = sorted(range(len(send_order)), key=lambda place: send_order[place])
    counts = [counts_ref[r : r + 1, :][0, 0] for r in range(owned)]
    copies = []
    slot = 0
    for r in range(owned):
        parts = []
        for k in range(PB):
            at = pl.multiple_of(jnp.minimum(slot + k, used - 1) * BLK, BLK)
            part = rows_ref[:, pl.ds(at, BLK)]
            parts.append(jnp.where(counts[r] > k, part, jnp.zeros_like(part)))
        slot = slot + counts[r]
        rows = jnp.concatenate(parts, axis=1)
        pair = jnp.dot(rows, coef_ref[r], preferred_element_type=jnp.float32)
        groups = [pair[place * row_total : (place + 1) * row_total] for place in places]
        pair_ref[r] = jnp.concatenate(groups, axis=0).astype(jnp.bfloat16)
        copies.append(pltpu.make_async_copy(pair_ref.at[r], pair_hbm.at[r], sems.at[owned + r]))
        copies[-1].start()
    for r in range(owned):
        pair = pair_ref[r]
        metric = lax.dot_general(
            pair, pair, (((0,), (0,)), ((), ())), preferred_element_type=jnp.float32
        )
        metric_ref[r] = metric / aux_total
        copies.append(pltpu.make_async_copy(metric_ref.at[r], metric_hbm.at[r], sems.at[r]))
        copies[-1].start()
    for copy in copies:
        copy.wait()


def shards(aux_ints, lmo_coef, ao_domain, ao_count, pao_domain, pao_count, owner_order, pao_coef):
    devices = lax.axis_size(AXES)
    rows_each = lmo_coef.shape[0]
    lmo_total = devices * rows_each
    row_total, ao_total, _ = aux_ints.shape
    owned = pao_coef.shape[0]
    aux_total = devices * row_total
    cols = devices * USED

    vmem = pl.BlockSpec(memory_space=pltpu.VMEM)
    small = pltpu.CompilerParams(vmem_limit_bytes=16 * 2**20)
    bcast = pl.pallas_call(
        spread_kernel,
        out_shape=jax.ShapeDtypeStruct((devices,) + lmo_coef.shape, jnp.bfloat16),
        in_specs=[pl.BlockSpec(memory_space=pltpu.HBM)],
        out_specs=vmem,
        scratch_shapes=[pltpu.VMEM(lmo_coef.shape, jnp.bfloat16), pltpu.SemaphoreType.DMA],
        compiler_params=small,
        cost_estimate=pl.CostEstimate(flops=2 * 10**10, bytes_accessed=2**18, transcendentals=0),
        name="spread",
    )(pltpu.with_memory_space_constraint(lmo_coef, pltpu.HBM))
    gather_order = participants(GATHER_ORDER, devices)
    send_order = participants(SEND_ORDER, devices)
    coef = exchange(bcast, gather_order)
    send, counts = pl.pallas_call(
        lambda *refs: half_kernel(owned, gather_order, send_order, *refs),
        out_shape=(
            jax.ShapeDtypeStruct((devices, row_total, USED * BLK), jnp.bfloat16),
            jax.ShapeDtypeStruct((owned, 128), jnp.int32),
        ),
        in_specs=[vmem] * 7,
        out_specs=(vmem,) * 2,
        scratch_shapes=[
            pltpu.VMEM((lmo_total, DB * BLK), jnp.float32),
            pltpu.VMEM((cols * row_total, BLK), jnp.float32),
        ],
        compiler_params=pltpu.CompilerParams(vmem_limit_bytes=24 * 2**20),
        cost_estimate=pl.CostEstimate(
            flops=2 * row_total * ao_total * ao_total * cols, bytes_accessed=2 * aux_ints.size, transcendentals=0
        ),
        name="half_transform",
    )(aux_ints, coef, ao_domain.T, ao_count[None], pao_domain.T, pao_count[None], owner_order[None])
    received = exchange(send, send_order)
    outs = (
        ((owned, aux_total, pao_coef.shape[2]), jnp.bfloat16),
        ((owned, pao_coef.shape[2], pao_coef.shape[2]), jnp.float32),
    )
    return pl.pallas_call(
        lambda *refs: pair_kernel(send_order, *refs),
        out_shape=tuple(jax.ShapeDtypeStruct(*out) for out in outs),
        in_specs=[vmem] * 3,
        out_specs=(pl.BlockSpec(memory_space=pltpu.HBM),) * 2,
        scratch_shapes=[pltpu.VMEM(*out) for out in outs] + [pltpu.SemaphoreType.DMA((2 * owned,))],
        compiler_params=small,
        name="pair_transform",
    )(counts, received.reshape(aux_total, USED * BLK), pao_coef)


def solution(mesh):
    placed = (
        P(AXES, None, None),
        P(AXES, None),
        P(),
        P(),
        P(),
        P(),
        P(),
        P(AXES, None, None),
    )
    return jax.shard_map(
        shards,
        mesh=mesh,
        in_specs=placed,
        out_specs=(P(AXES, None, None), P(AXES, None, None)),
        check_vma=False,
    )
```

```python
import jax
import jax.numpy as jnp
from jax import lax
from jax.experimental import pallas as pl
from jax.experimental.pallas import tpu as pltpu
from jax.sharding import PartitionSpec as P

BLK = 128
DB = 3
PB = 3
USED = 8
AXES = ("aux", "lmo")

GATHER_ORDER = (
    11, 0, 25, 21, 31, 22, 5, 20, 14, 30, 13, 16, 9, 7, 17, 1, 15, 12, 4, 2, 10, 3, 18, 19,
    27, 24, 29, 6, 8, 28, 26, 23,
)
SEND_ORDER = (
    24, 27, 5, 30, 1, 19, 25, 26, 16, 2, 12, 18, 14, 6, 7, 9, 22, 8, 4, 11, 3, 20, 0, 21, 10,
    29, 28, 23, 31, 13, 17, 15,
)


def participants(order, devices):
    rank = {device: place for place, device in enumerate(order)}
    return sorted(range(devices), key=lambda device: (rank[device % len(order)], device))


def exchange(blocks, order):
    return lax.all_to_all(
        blocks, AXES, split_axis=0, concat_axis=0, tiled=True, axis_index_groups=[order]
    )


def spread_kernel(coef_hbm, bcast_ref, coef_ref, sem):
    copy = pltpu.make_async_copy(coef_hbm, coef_ref, sem)
    copy.start()
    copy.wait()
    own = coef_ref[...]
    for dev in range(bcast_ref.shape[0]):
        bcast_ref[dev] = own


def rows_of(row, count):
    return jnp.broadcast_to(row, (count, row.shape[1])).astype(jnp.bfloat16)


def half_kernel(
    owned, gather_order, send_order,
    aux_ref, coef_ref, ao_dom_ref, ao_cnt_ref, pao_dom_ref, pao_cnt_ref, order_ref,
    send_ref, counts_ref, flat_ref, tiles_ref,
):
    rows_each = coef_ref.shape[1]
    lmo_total = order_ref.shape[1]
    devices, row_total, width = send_ref.shape
    used = width // BLK
    cols = devices * used
    blocks = aux_ref.shape[1] // BLK

    lmo_id = lax.broadcasted_iota(jnp.int32, (lmo_total, lmo_total), 0)
    held = jnp.where(order_ref[...] == lmo_id, 1.0, 0.0).astype(jnp.bfloat16)
    cnt_slot = jnp.dot(
        rows_of(pao_cnt_ref[...], 8), held, preferred_element_type=jnp.float32
    )[:1].astype(jnp.int32)
    slot_id = lax.broadcasted_iota(jnp.int32, (1, lmo_total), 1)
    member = slot_id % owned
    base = jnp.zeros_like(cnt_slot)
    for step in range(1, owned):
        base = base + jnp.where(member >= step, pltpu.roll(cnt_slot, step, 1), 0)
    facts = jnp.concatenate(
        [rows_of(fact, 128) for fact in (slot_id // owned, base, cnt_slot)], axis=0
    )
    facts = lax.dot_general(
        held, facts, (((1,), (1,)), ((), ())), preferred_element_type=jnp.float32
    ).astype(jnp.int32)
    first = facts[:, :128] * used + facts[:, 128:256]
    count = facts[:, 256:]

    lane = lax.broadcasted_iota(jnp.int32, (lmo_total, 128), 1)
    spread = []
    for part in range(cols // 128):
        place = lane + part * 128 - first
        spread.append(jnp.where((place >= 0) & (place < count), 1.0, 0.0))
    spread = jnp.concatenate(spread, axis=1).astype(jnp.bfloat16)

    by_lmo = lax.dot_general(
        jnp.concatenate([rows_of(fact, 16) for fact in (slot_id // owned, base)], axis=0),
        held, (((1,), (1,)), ((), ())), preferred_element_type=jnp.float32,
    ).astype(jnp.bfloat16)
    by_lmo = jnp.concatenate(
        [by_lmo] + [rows_of(pao_dom_ref[k : k + 1, :], 16) for k in range(PB)], axis=0
    )
    by_col = jnp.dot(by_lmo, spread, preferred_element_type=jnp.float32)
    by_col = [by_col[16 * n : 16 * n + 1] for n in range(2 + PB)]
    col_id = lax.broadcasted_iota(jnp.int32, (1, cols), 1).astype(jnp.float32)
    place = col_id - (by_col[0] * used + by_col[1])
    block_row = by_col[2]
    for k in range(1, PB):
        block_row = jnp.where(place >= k, by_col[2 + k], block_row)

    for place, src in enumerate(gather_order):
        flat_ref[pl.ds(src * rows_each, rows_each), :] = coef_ref[place].astype(jnp.float32)
    coef_t = flat_ref[...].T
    homes = [
        jnp.where(ao_cnt_ref[...] > k, ao_dom_ref[k : k + 1, :], -1) for k in range(DB)
    ]
    dense = []
    for b in range(blocks):
        total = jnp.zeros((BLK, lmo_total), jnp.float32)
        for k in range(DB):
            total = jnp.where(homes[k] == b, coef_t[k * BLK : (k + 1) * BLK, :], total)
        dense.append(total)
    weights = []
    for b in range(0, blocks, 2):
        dense_t = jnp.concatenate(dense[b : b + 2], axis=0).astype(jnp.bfloat16)
        weights.append(
            jnp.dot(dense_t, spread, preferred_element_type=jnp.float32).astype(jnp.bfloat16)
        )

    for p in range(row_total):
        half = sum(
            jnp.dot(
                aux_ref[p, :, 2 * BLK * n : 2 * BLK * (n + 1)],
                weight,
                preferred_element_type=jnp.float32,
            )
            for n, weight in enumerate(weights)
        )
        picked = half[:BLK]
        for b in range(1, blocks):
            picked = jnp.where(block_row == b, half[b * BLK : (b + 1) * BLK], picked)
        tiles_ref[pl.ds(p, cols, stride=row_total), :] = picked.T
    mine = lax.axis_index(AXES) * owned
    for r in range(owned):
        here = jnp.where(slot_id == mine + r, cnt_slot, 0).astype(jnp.float32)
        here = jnp.sum(here, axis=1, keepdims=True).astype(jnp.int32)
        counts_ref[r : r + 1, :] = jnp.broadcast_to(here, (1, 128))
    for place, dev in enumerate(send_order):
        for slot in range(used):
            tile = tiles_ref[pl.ds((dev * used + slot) * row_total, row_total), :]
            send_ref[place, :, slot * BLK : (slot + 1) * BLK] = tile.astype(jnp.bfloat16)


def pair_kernel(send_order, counts_ref, rows_ref, coef_ref, pair_hbm, metric_hbm, pair_ref, metric_ref, sems):
    owned, aux_total, _ = pair_ref.shape
    used = rows_ref.shape[1] // BLK
    row_total = aux_total // len(send_order)
    places = sorted(range(len(send_order)), key=lambda place: send_order[place])
    counts = [counts_ref[r : r + 1, :][0, 0] for r in range(owned)]
    copies = []
    slot = 0
    for r in range(owned):
        parts = []
        for k in range(PB):
            at = pl.multiple_of(jnp.minimum(slot + k, used - 1) * BLK, BLK)
            part = rows_ref[:, pl.ds(at, BLK)]
            parts.append(jnp.where(counts[r] > k, part, jnp.zeros_like(part)))
        slot = slot + counts[r]
        rows = jnp.concatenate(parts, axis=1)
        pair = jnp.dot(rows, coef_ref[r], preferred_element_type=jnp.float32)
        groups = [pair[place * row_total : (place + 1) * row_total] for place in places]
        pair_ref[r] = jnp.concatenate(groups, axis=0).astype(jnp.bfloat16)
        copies.append(pltpu.make_async_copy(pair_ref.at[r], pair_hbm.at[r], sems.at[owned + r]))
        copies[-1].start()
    for r in range(owned):
        pair = pair_ref[r]
        metric = lax.dot_general(
            pair, pair, (((0,), (0,)), ((), ())), preferred_element_type=jnp.float32
        )
        metric_ref[r] = metric / aux_total
        copies.append(pltpu.make_async_copy(metric_ref.at[r], metric_hbm.at[r], sems.at[r]))
        copies[-1].start()
    for copy in copies:
        copy.wait()


def shards(aux_ints, lmo_coef, ao_domain, ao_count, pao_domain, pao_count, owner_order, pao_coef):
    devices = lax.axis_size(AXES)
    rows_each = lmo_coef.shape[0]
    lmo_total = devices * rows_each
    row_total, ao_total, _ = aux_ints.shape
    owned = pao_coef.shape[0]
    aux_total = devices * row_total
    cols = devices * USED

    vmem = pl.BlockSpec(memory_space=pltpu.VMEM)
    small = pltpu.CompilerParams(vmem_limit_bytes=16 * 2**20)
    bcast = pl.pallas_call(
        spread_kernel,
        out_shape=jax.ShapeDtypeStruct((devices,) + lmo_coef.shape, jnp.bfloat16),
        in_specs=[pl.BlockSpec(memory_space=pltpu.HBM)],
        out_specs=vmem,
        scratch_shapes=[pltpu.VMEM(lmo_coef.shape, jnp.bfloat16), pltpu.SemaphoreType.DMA],
        compiler_params=small,
        cost_estimate=pl.CostEstimate(flops=2 * 10**10, bytes_accessed=2**18, transcendentals=0),
        name="spread",
    )(pltpu.with_memory_space_constraint(lmo_coef, pltpu.HBM))
    gather_order = participants(GATHER_ORDER, devices)
    send_order = participants(SEND_ORDER, devices)
    coef = exchange(bcast, gather_order)
    send, counts = pl.pallas_call(
        lambda *refs: half_kernel(owned, gather_order, send_order, *refs),
        out_shape=(
            jax.ShapeDtypeStruct((devices, row_total, USED * BLK), jnp.bfloat16),
            jax.ShapeDtypeStruct((owned, 128), jnp.int32),
        ),
        in_specs=[vmem] * 7,
        out_specs=(vmem,) * 2,
        scratch_shapes=[
            pltpu.VMEM((lmo_total, DB * BLK), jnp.float32),
            pltpu.VMEM((cols * row_total, BLK), jnp.float32),
        ],
        compiler_params=pltpu.CompilerParams(vmem_limit_bytes=24 * 2**20),
        cost_estimate=pl.CostEstimate(
            flops=2 * row_total * ao_total * ao_total * cols, bytes_accessed=2 * aux_ints.size, transcendentals=0
        ),
        name="half_transform",
    )(aux_ints, coef, ao_domain.T, ao_count[None], pao_domain.T, pao_count[None], owner_order[None])
    received = exchange(send, send_order)
    outs = (
        ((owned, aux_total, pao_coef.shape[2]), jnp.bfloat16),
        ((owned, pao_coef.shape[2], pao_coef.shape[2]), jnp.float32),
    )
    return pl.pallas_call(
        lambda *refs: pair_kernel(send_order, *refs),
        out_shape=tuple(jax.ShapeDtypeStruct(*out) for out in outs),
        in_specs=[vmem] * 3,
        out_specs=(pl.BlockSpec(memory_space=pltpu.HBM),) * 2,
        scratch_shapes=[pltpu.VMEM(*out) for out in outs] + [pltpu.SemaphoreType.DMA((2 * owned,))],
        compiler_params=small,
        name="pair_transform",
    )(counts, received.reshape(aux_total, USED * BLK), pao_coef)


def solution(mesh):
    placed = (
        P(AXES, None, None),
        P(AXES, None),
        P(),
        P(),
        P(),
        P(),
        P(),
        P(AXES, None, None),
    )
    return jax.shard_map(
        shards,
        mesh=mesh,
        in_specs=placed,
        out_specs=(P(AXES, None, None), P(AXES, None, None)),
        check_vma=False,
    )
```
